256 devices in a mesh: chan: 8 (over z_hi, x), clus: 32 (over z_lo, y, core).
Axes of the slice: x: 4, y: 4, z: 8 (z_hi: 2, z_lo: 4; z = z_hi * 4 + z_lo), core: 2. Of those that a mesh axis runs over, the one named last changes fastest.
Arguments:
- waveform: float32 [88, 1280], P('chan', 'clus'), may hold values from -33 to 33
- basis_slots: bfloat16 [88, 128, 8, 1024], P('chan', 'clus'), may hold values from -0.1875 to 0.1875
- slot_channel: int32 [88], P('chan'), may hold values from 0 to 87, as said below
- cluster_holder: int32 [64], replicated, may hold values from 0 to 31, as said below
- basis_count: int32 [64], replicated, may hold values from 1 to 8
Outputs:
- detection: float32 [64, 256], P('clus', 'chan')
The draws below stay inside these ranges and needn't reach their ends.
Inputs may be any that keep to these rules, and one draw needn't show every extreme that they name: `slot_channel`: each aligned block of 11 entries holds the channel numbers of the same block, each once. `cluster_holder`: no index is named by more than 4 clusters and some index by exactly 4. Among the clusters c with the same c // 2, no index is named more than 2 times, and every index that is named is named exactly 2 times.
All inputs are finite; a program needn't handle non-finite values.
Results may differ from the reference program's by a relative error of at most 0.00045.
Values sent between devices are 32-bit elements; how exact they have to be, the bound alone decides.
A program may use at most 64 MiB of HBM per device.

```python
import jax
import jax.numpy as jnp
from jax import lax

CHANNELS = 88
WINDOW = 1024
RANK = 8
CAPACITY = 2
CL_DEV = 2
LAGS = 256
GROUP = 11
SLOTS = 4
CLUSTERS = 64
SLOT_ALL = 128
TIME_LEN = 1280


def draw_waveform(key, part):
    key_a, key_b = jax.random.split(jax.random.fold_in(key, 11), 2)
    level = 3.0 ** (jnp.arange(CHANNELS, dtype=jnp.float32) / (CHANNELS - 1))
    jitter = jax.random.uniform(key_a, (CHANNELS,), jnp.float32, 0.7, 1.4)
    noise = jnp.clip(jax.random.normal(key_b, (CHANNELS, TIME_LEN), jnp.float32), -6.0, 6.0)
    return (noise * (level * jitter)[:, None]).astype(jnp.float32)


def draw_slot_channel(key, part):
    groups = CHANNELS // GROUP
    key_list = jax.random.split(jax.random.fold_in(key, 23), groups)

    def shuffle(single_key):
        return jax.random.permutation(single_key, GROUP)
    shuffled = jax.vmap(shuffle)(key_list)
    offsets = jnp.arange(groups, dtype=jnp.int32)[:, None] * GROUP
    return (shuffled.astype(jnp.int32) + offsets).reshape(-1).astype(jnp.int32)


def draw_cluster_holder(key, part):
    holders = CLUSTERS // CL_DEV
    half_count = holders // 2
    pair_count = CL_DEV // CAPACITY
    key_a, key_b, key_c = jax.random.split(jax.random.fold_in(key, 37), 3)
    device_order = jax.random.permutation(key_a, holders).astype(jnp.int32)
    sides = jax.random.randint(key_b, (holders, pair_count), 0, 2).astype(jnp.int32)
    owner_ids = jnp.arange(holders, dtype=jnp.int32)[:, None]
    pair_ids = jnp.arange(pair_count, dtype=jnp.int32)[None, :]
    target = (pair_count * owner_ids + pair_ids) % half_count
    sides = jnp.where(target == 0, 0, sides)
    devices = device_order[target + half_count * sides]

    def shuffle(single_key):
        return jax.random.permutation(single_key, CL_DEV)
    shuffled = jax.vmap(shuffle)(jax.random.split(key_c, holders)).astype(jnp.int32)
    chosen = jnp.take_along_axis(devices, shuffled // CAPACITY, axis=1)
    return chosen.reshape(-1).astype(jnp.int32)


def place_ends(entries, rng, low, top_value):
    shape = entries.shape
    index_at = [jax.random.randint(jax.random.fold_in(rng, axis), (), 0, shape[axis]) for axis in range(len(shape))]
    entries = entries.at[tuple(index_at)].set(low)
    longest = shape.index(max(shape))
    index_at[longest] = (index_at[longest] + 1) % shape[longest]
    return entries.at[tuple(index_at)].set(top_value)


def block_levels(own_key, extent, cuts, least, high):
    level, own = 1.0, jax.random.fold_in(own_key, 6)
    for dim, parts in cuts:
        heights = jnp.exp(jax.random.uniform(jax.random.fold_in(own, dim), (parts,), jnp.float32, least / len(cuts), high / len(cuts)))
        level = level * jnp.repeat(heights, extent[dim] // parts).reshape([-1 if axis == dim else 1 for axis in range(len(extent))])
    return level


def scatter_about(own_key, shape, scale, most, cuts=(), kind=jnp.bfloat16):
    values = jax.random.normal(own_key, shape, jnp.float32) * scale
    if len(cuts) > 0:
        values = block_levels(own_key, shape, cuts, -0.22, 0.18) * values
    return jnp.clip(values, min=-most, max=most).astype(kind)


def setup_inputs(seed: int = 0) -> dict:
    key_of = jax.random.split(jax.random.key(seed), 6)
    return {
        "waveform": draw_waveform(jax.random.fold_in(key_of[5], 71), 0),
        "basis_slots": scatter_about(key_of[1], (CHANNELS, SLOT_ALL, RANK, WINDOW), WINDOW ** -0.5, 0.1875, ((0, 8), (1, 32))),
        "slot_channel": draw_slot_channel(jax.random.fold_in(key_of[5], 71), 0),
        "cluster_holder": draw_cluster_holder(jax.random.fold_in(key_of[5], 71), 0),
        "basis_count": place_ends(jax.random.randint(key_of[4], (CLUSTERS,), 1, RANK + 1), jax.random.fold_in(key_of[4], 1), 1, RANK).astype(jnp.int32),
    }


def correlate(channel_row, filters, lag_count):
    signal = channel_row.reshape(1, 1, channel_row.shape[0])
    kernel = filters.reshape(filters.shape[0], 1, filters.shape[1])
    result = lax.conv_general_dilated(signal, kernel, (1,), "VALID", dimension_numbers=("NCH", "OIH", "NCH"), preferred_element_type=jnp.float32)
    return result[0, :, :lag_count]


def reference(waveform, basis_slots, slot_channel, cluster_holder, basis_count):
    ordered = jnp.zeros_like(waveform).at[slot_channel].set(waveform)
    rounded = ordered.astype(jnp.bfloat16)
    cluster_ids = jnp.arange(CLUSTERS, dtype=jnp.int32)
    same_holder = cluster_holder[:, None] == cluster_holder[None, :]
    earlier = cluster_ids[None, :] < cluster_ids[:, None]
    position = jnp.sum(same_holder & earlier, axis=1).astype(jnp.int32)
    slot_index = (cluster_holder * SLOTS + position).astype(jnp.int32)
    rank_mask = (jnp.arange(RANK, dtype=jnp.int32)[None, :] < basis_count[:, None]).astype(jnp.float32)

    def advance(running, inputs):
        basis_rows, channel_row = inputs
        chosen = jnp.take(basis_rows, slot_index, axis=0).reshape(CLUSTERS * RANK, WINDOW)
        projected = correlate(channel_row, chosen, LAGS)
        projected = projected.reshape(CLUSTERS, RANK, LAGS)
        return running + jnp.sum(projected * projected * rank_mask[:, :, None], axis=1), None

    captured, _ = lax.scan(advance, jnp.zeros((CLUSTERS, LAGS), jnp.float32), (basis_slots, rounded))
    squares = jnp.sum(ordered * ordered, axis=0)
    running_sum = jnp.concatenate([jnp.zeros((1,), squares.dtype), jnp.cumsum(squares)])
    energy = running_sum[WINDOW:WINDOW + LAGS] - running_sum[:LAGS]
    return (WINDOW / RANK) * captured / (energy[None, :] + 1e-6)
```

```python
import jax
import jax.numpy as jnp
from jax import lax
from jax.experimental import pallas as pl
from jax.experimental.pallas import tpu as pltpu
from jax.sharding import PartitionSpec as P

MESH = pl.DeviceIdType.MESH

X, Z_HI, Z_LO, Y, CORE = 4, 2, 4, 4, 2
CLUS = Z_LO * Y * CORE
CHANS = 11
PIECE = 40
LANES = 128
LAGS = 256
WINDOW = 1024
RANK = 8
SLOTS = 4
CLUSTERS = 64
CHUNKS = 10
HANKELS = 9


def clus_steps():
    steps = [(dz, dy, dc) for dz in range(Z_LO) for dy in range(Y) for dc in range(CORE)]
    steps.remove((0, 0, 0))

    def distance(step):
        dz, dy, dc = step
        return (0, 2, 2, 2)[dz] + (0, 1, 2, 1)[dy] + 0.1 * dc

    return sorted(steps, key=distance, reverse=True)


def far_steps():
    steps = [(dh, *rest) for dh in range(Z_HI) for rest in [(0, 0, 0), *clus_steps()]]
    steps.remove((0, 0, 0, 0))

    def distance(step):
        dh, dz, dy, dc = step
        return 2 * dh + (0, 2, 2, 2)[dz] + (0, 1, 2, 1)[dy] + 0.1 * dc

    return sorted(steps, key=distance, reverse=True)


def kernel(
    wave_hbm, basis_hbm, slot_hbm, holder_hbm, count_hbm, out_ref,
    wave_v, basis_v, slot_s, holder_s, count_s,
    pieces, record, hankel, squares_v, tx_a, rx_a, tx_b, rx_b, tx_e, rx_e,
    load_sem, send_1, recv_1, send_a, recv_a, send_b, recv_b, send_e, recv_e,
):
    chan = lax.axis_index("chan")
    clus = lax.axis_index("clus")
    z_hi, x = chan // X, chan % X
    z_lo, y, core = clus // (Y * CORE), (clus // CORE) % Y, clus % CORE

    def clus_at(dz, dy, dc):
        return ((z_lo + dz) % Z_LO) * (Y * CORE) + ((y + dy) % Y) * CORE + (core + dc) % CORE

    def chan_at(dh, dx):
        return ((z_hi + dh) % Z_HI) * X + (x + dx) % X

    loads = [
        pltpu.make_async_copy(source, target, load_sem.at[n])
        for n, (source, target) in enumerate(
            [(wave_hbm, wave_v), (basis_hbm, basis_v), (slot_hbm, slot_s), (holder_hbm, holder_s), (count_hbm, count_s)]
        )
    ]
    loads[0].start()

    barrier = pltpu.get_barrier_semaphore()
    greeted = [(chan, clus_at(*step)) for step in clus_steps()]
    greeted += [(chan_at(0, dx), clus) for dx in (2, 1, 3)]
    greeted += [(chan_at(1, 0), clus)]
    for device in greeted:
        pl.semaphore_signal(barrier, inc=1, device_id=device, device_id_type=MESH)
    for load in loads[1:]:
        load.start()

    loads[0].wait()
    from_id = lax.broadcasted_iota(jnp.int32, (PIECE, PIECE), 0)
    to_id = lax.broadcasted_iota(jnp.int32, (PIECE, PIECE), 1)
    turn = jnp.where(from_id + to_id == PIECE - 1, 1.0, 0.0).astype(jnp.float32)
    turned = jnp.dot(wave_v[...], turn, precision=lax.Precision.HIGHEST, preferred_element_type=jnp.float32)
    pieces[clus] = jnp.zeros((4, LANES), jnp.float32)
    pieces[clus, :, 0:PIECE] = turned[0:4, :]
    pieces[clus, :, PIECE : 2 * PIECE] = turned[4:8, :]
    pieces[clus, 0:3, 2 * PIECE : 3 * PIECE] = turned[8:11, :]
    pl.semaphore_wait(barrier, len(greeted))

    for step in clus_steps():
        pltpu.make_async_remote_copy(
            src_ref=pieces.at[clus], dst_ref=pieces.at[clus], send_sem=send_1, recv_sem=recv_1,
            device_id=(chan, clus_at(*step)), device_id_type=MESH,
        ).start()

    for load in loads[1:]:
        load.wait()
    own = [2 * clus, 2 * clus + 1]
    own_holder = [holder_s[c] for c in own]

    def count_cluster(c, carry):
        held, ranks, positions = carry
        holder, rank = holder_s[c], count_s[c]
        mine = holder == clus
        ranks = tuple(
            r + jnp.where(jnp.logical_and(mine, held == p), rank, 0) for p, r in enumerate(ranks)
        )
        positions = tuple(
            n + jnp.where(jnp.logical_and(holder == h, c < o), 1, 0)
            for n, h, o in zip(positions, own_holder, own)
        )
        return held + jnp.where(mine, 1, 0), ranks, positions

    zero = jnp.int32(0)
    _, ranks, positions = lax.fori_loop(
        0, CLUSTERS, count_cluster, (zero, (zero,) * SLOTS, (zero,) * 2)
    )

    pltpu.make_async_copy(pieces.at[pl.ds(0, CLUS - 1)], pieces.at[pl.ds(0, CLUS - 1)], recv_1).wait()

    lane = lax.broadcasted_iota(jnp.int32, (4, LANES), 1)
    squares_v[...] = jnp.zeros((16, LANES), jnp.float32)
    for c in range(CHUNKS):
        rows = [jnp.zeros((4, LANES), jnp.float32)] * 3
        for i in range(CLUS):
            low = LANES * (c + 1) - PIECE * (i + 1)
            high = low + PIECE
            if high <= 0 or low >= LANES:
                continue
            inside = (lane >= low) & (lane < high)
            piece = pieces[i]
            for a in range(3):
                moved = pltpu.roll(piece, (low - PIECE * a) % LANES, 1)
                rows[a] = jnp.where(inside, moved, rows[a])
        for a in range(3):
            record[c, 4 * a : 4 * a + 4, :] = rows[a]
        total = jnp.sum(rows[0] * rows[0] + rows[1] * rows[1] + rows[2] * rows[2], axis=0, keepdims=True)
        squares_v[c : c + 1, :] = total

    squares = squares_v[...]
    row_id = lax.broadcasted_iota(jnp.int32, (LANES, LANES), 0)
    col_id = lax.broadcasted_iota(jnp.int32, (LANES, LANES), 1)
    upto = jnp.where(row_id <= col_id, 1.0, 0.0).astype(jnp.float32)
    prefix = jnp.dot(squares, upto, precision=lax.Precision.HIGHEST, preferred_element_type=jnp.float32)
    energy = []
    for h in range(2):
        whole = jnp.sum(prefix[h + 1 : h + 9, LANES - 1 : LANES], axis=0, keepdims=True)
        energy.append(prefix[h : h + 1, :] + (whole - prefix[h + 8 : h + 9, :]))

    near = row_id <= col_id
    captured = jnp.zeros((SLOTS * RANK, LAGS), jnp.float32)
    for j in range(CHANS):
        rolled = None
        for c in range(CHUNKS):
            later = pltpu.roll(
                jnp.broadcast_to(record[c, j : j + 1, :], (LANES, LANES)), 0, 1, stride=1, stride_axis=0
            )
            if c > 0:
                block = jnp.where(near, rolled, later)
                hankel[j, LANES * (c - 1) : LANES * c, :] = block.astype(jnp.bfloat16)
            rolled = later
        vectors = basis_v[lax.rem(slot_s[j], CHANS)]
        windows = jnp.concatenate([hankel[j, 0:WINDOW, :], hankel[j, LANES : LANES + WINDOW, :]], axis=1)
        projected = jnp.dot(vectors, windows, preferred_element_type=jnp.float32)
        captured = captured + projected * projected

    rank_id = lax.broadcasted_iota(jnp.int32, (RANK, LAGS), 0)
    tx_a[...] = jnp.zeros((X, 4, LANES), jnp.float32)
    for p in range(SLOTS):
        part = jnp.where(rank_id < ranks[p], captured[RANK * p : RANK * (p + 1), :], 0.0)
        row = jnp.sum(part, axis=0, keepdims=True)
        for h in range(2):
            for v in range(X):
                start = LANES * h + 32 * (X - 1 - v)
                tx_a[v, h : h + 1, 32 * p : 32 * (p + 1)] = row[:, start : start + 32]
    for h in range(2):
        for v in range(X):
            start = 32 * (X - 1 - v)
            tx_a[v, 2:3, 32 * h : 32 * (h + 1)] = energy[h][:, start : start + 32]

    for dx in (2, 1, 3):
        pltpu.make_async_remote_copy(
            src_ref=tx_a.at[(x + dx) % X], dst_ref=rx_a.at[x], send_sem=send_a, recv_sem=recv_a,
            device_id=(chan_at(0, dx), clus), device_id_type=MESH,
        ).start()
    rx_a[x] = tx_a[x]
    pltpu.make_async_copy(rx_a.at[pl.ds(0, X - 1)], rx_a.at[pl.ds(0, X - 1)], recv_a).wait()
    reduced = rx_a[0] + rx_a[1] + rx_a[2] + rx_a[3]

    tx_b[0] = reduced[0:1, :]
    tx_b[1] = reduced[1:2, :]
    tx_e[...] = reduced[2:3, :]
    me = z_hi * CLUS + clus
    energy_copy = pltpu.make_async_remote_copy(
        src_ref=tx_e, dst_ref=rx_e, send_sem=send_e, recv_sem=recv_e,
        device_id=(chan_at(1, 0), clus), device_id_type=MESH,
    )
    energy_copy.start()
    for dh, *step in far_steps():
        pltpu.make_async_remote_copy(
            src_ref=tx_b.at[(z_hi + dh) % Z_HI], dst_ref=rx_b.at[me], send_sem=send_b, recv_sem=recv_b,
            device_id=(chan_at(dh, 0), clus_at(*step)), device_id_type=MESH,
        ).start()
    rx_b[me] = tx_b[z_hi]
    energy_copy.wait_recv()
    both = reduced[2:3, :] + rx_e[...]
    energy_own = jnp.where(z_hi == 0, both[:, 0:32], both[:, 32:64]) + 1e-6
    pltpu.make_async_copy(rx_b.at[pl.ds(0, 2 * CLUS - 1)], rx_b.at[pl.ds(0, 2 * CLUS - 1)], recv_b).wait()
    for q in range(2):
        row = rx_b[own_holder[q]] + rx_b[CLUS + own_holder[q]]
        value = jnp.zeros((1, 32), jnp.float32)
        for p in range(SLOTS):
            value = jnp.where(positions[q] == p, row[:, 32 * p : 32 * (p + 1)], value)
        out_ref[q : q + 1, :] = (WINDOW / RANK) * value / energy_own

    pltpu.make_async_copy(pieces.at[pl.ds(0, CLUS - 1)], pieces.at[pl.ds(0, CLUS - 1)], send_1).wait()
    pltpu.make_async_copy(rx_a.at[pl.ds(0, X - 1)], rx_a.at[pl.ds(0, X - 1)], send_a).wait()
    pltpu.make_async_copy(rx_b.at[pl.ds(0, 2 * CLUS - 1)], rx_b.at[pl.ds(0, 2 * CLUS - 1)], send_b).wait()
    energy_copy.wait_send()


def local(waveform, basis_slots, slot_channel, cluster_holder, basis_count):
    basis = basis_slots.reshape(CHANS, SLOTS * RANK, WINDOW)
    f32 = jnp.float32
    latest_first = pl.pallas_call(
        kernel,
        out_shape=jax.ShapeDtypeStruct((2, 32), f32),
        in_specs=[pl.BlockSpec(memory_space=pltpu.HBM)] * 5,
        out_specs=pl.BlockSpec(memory_space=pltpu.VMEM),
        scratch_shapes=[
            pltpu.VMEM((CHANS, PIECE), f32),
            pltpu.VMEM((CHANS, SLOTS * RANK, WINDOW), jnp.bfloat16),
            pltpu.SMEM((CHANS,), jnp.int32),
            pltpu.SMEM((CLUSTERS,), jnp.int32),
            pltpu.SMEM((CLUSTERS,), jnp.int32),
            pltpu.VMEM((CLUS, 4, LANES), f32),
            pltpu.VMEM((CHUNKS, 16, LANES), f32),
            pltpu.VMEM((CHANS, HANKELS * LANES, LANES), jnp.bfloat16),
            pltpu.VMEM((16, LANES), f32),
            pltpu.VMEM((X, 4, LANES), f32),
            pltpu.VMEM((X, 4, LANES), f32),
            pltpu.VMEM((Z_HI, 1, LANES), f32),
            pltpu.VMEM((Z_HI * CLUS, 1, LANES), f32),
            pltpu.VMEM((1, LANES), f32),
            pltpu.VMEM((1, LANES), f32),
            pltpu.SemaphoreType.DMA((5,)),
            *[pltpu.SemaphoreType.DMA] * 8,
        ],
        compiler_params=pltpu.CompilerParams(collective_id=0, has_side_effects=True),
    )(waveform, basis, slot_channel, cluster_holder, basis_count)
    return latest_first[:, ::-1]


def solution(mesh):
    placed = (P("chan", "clus"), P("chan", "clus", None, None), P("chan"), P(), P())
    return jax.shard_map(
        local, mesh=mesh, in_specs=placed, out_specs=P("clus", "chan"), check_vma=False
    )
```

```python
import jax
import jax.numpy as jnp
from jax import lax
from jax.experimental import pallas as pl
from jax.experimental.pallas import tpu as pltpu
from jax.sharding import PartitionSpec as P

MESH = pl.DeviceIdType.MESH

X, Z_HI, Z_LO, Y, CORE = 4, 2, 4, 4, 2
CLUS = Z_LO * Y * CORE
CHANS = 11
PIECE = 40
LANES = 128
LAGS = 256
WINDOW = 1024
RANK = 8
SLOTS = 4
CLUSTERS = 64
CHUNKS = 10
HANKELS = 9


def clus_steps():
    steps = [(dz, dy, dc) for dz in range(Z_LO) for dy in range(Y) for dc in range(CORE)]
    steps.remove((0, 0, 0))

    def distance(step):
        dz, dy, dc = step
        return (0, 2, 2, 2)[dz] + (0, 1, 2, 1)[dy] + 0.1 * dc

    return sorted(steps, key=distance, reverse=True)


def chip_steps():
    steps = [(dh, dz, dy) for dh in range(Z_HI) for dz in range(Z_LO) for dy in range(Y)]
    steps.remove((0, 0, 0))

    def distance(step):
        dh, dz, dy = step
        return 2 * dh + (0, 2, 2, 2)[dz] + (0, 1, 2, 1)[dy]

    return sorted(steps, key=distance, reverse=True)


X_STEPS = [(2, 1), (2, 0), (1, 1), (3, 1), (1, 0), (3, 0), (0, 1)]


def kernel(
    wave_hbm, basis_hbm, slot_hbm, holder_hbm, count_hbm, out_ref,
    wave_v, basis_v, slot_s, holder_s, count_s,
    pieces, record, hankel, squares_v, tx_a, rx_a, tx_b, rx_b, tx_e, rx_e,
    load_sem, send_1, recv_1, send_a, recv_a, send_b, recv_b, send_e, recv_e,
):
    chan = lax.axis_index("chan")
    clus = lax.axis_index("clus")
    z_hi, x = chan // X, chan % X
    z_lo, y, core = clus // (Y * CORE), (clus // CORE) % Y, clus % CORE

    def clus_at(dz, dy, dc):
        return ((z_lo + dz) % Z_LO) * (Y * CORE) + ((y + dy) % Y) * CORE + (core + dc) % CORE

    def chan_at(dh, dx):
        return ((z_hi + dh) % Z_HI) * X + (x + dx) % X

    loads = [
        pltpu.make_async_copy(source, target, load_sem.at[n])
        for n, (source, target) in enumerate(
            [(wave_hbm, wave_v), (basis_hbm, basis_v), (slot_hbm, slot_s), (holder_hbm, holder_s), (count_hbm, count_s)]
        )
    ]
    loads[0].start()

    barrier = pltpu.get_barrier_semaphore()
    greeted = [(chan, clus_at(*step)) for step in clus_steps()]
    greeted += [(chan_at(0, dx), clus_at(0, 0, dc)) for dx, dc in X_STEPS if dx > 0]
    greeted += [(chan_at(1, 0), clus)]
    for device in greeted:
        pl.semaphore_signal(barrier, inc=1, device_id=device, device_id_type=MESH)
    for load in loads[1:]:
        load.start()

    loads[0].wait()
    from_id = lax.broadcasted_iota(jnp.int32, (PIECE, PIECE), 0)
    to_id = lax.broadcasted_iota(jnp.int32, (PIECE, PIECE), 1)
    turn = jnp.where(from_id + to_id == PIECE - 1, 1.0, 0.0).astype(jnp.float32)
    turned = jnp.dot(wave_v[...], turn, precision=lax.Precision.HIGHEST, preferred_element_type=jnp.float32)
    pieces[clus] = jnp.zeros((4, LANES), jnp.float32)
    pieces[clus, :, 0:PIECE] = turned[0:4, :]
    pieces[clus, :, PIECE : 2 * PIECE] = turned[4:8, :]
    pieces[clus, 0:3, 2 * PIECE : 3 * PIECE] = turned[8:11, :]
    pl.semaphore_wait(barrier, len(greeted))

    for step in clus_steps():
        pltpu.make_async_remote_copy(
            src_ref=pieces.at[clus], dst_ref=pieces.at[clus], send_sem=send_1, recv_sem=recv_1,
            device_id=(chan, clus_at(*step)), device_id_type=MESH,
        ).start()

    for load in loads[1:]:
        load.wait()
    own = [2 * clus, 2 * clus + 1]
    own_holder = [holder_s[c] for c in own]

    def count_cluster(c, carry):
        held, ranks, positions = carry
        holder, rank = holder_s[c], count_s[c]
        mine = holder == clus
        ranks = tuple(
            r + jnp.where(jnp.logical_and(mine, held == p), rank, 0) for p, r in enumerate(ranks)
        )
        positions = tuple(
            n + jnp.where(jnp.logical_and(holder == h, c < o), 1, 0)
            for n, h, o in zip(positions, own_holder, own)
        )
        return held + jnp.where(mine, 1, 0), ranks, positions

    zero = jnp.int32(0)
    _, ranks, positions = lax.fori_loop(
        0, CLUSTERS, count_cluster, (zero, (zero,) * SLOTS, (zero,) * 2)
    )

    pltpu.make_async_copy(pieces.at[pl.ds(0, CLUS - 1)], pieces.at[pl.ds(0, CLUS - 1)], recv_1).wait()

    lane = lax.broadcasted_iota(jnp.int32, (4, LANES), 1)
    squares_v[...] = jnp.zeros((16, LANES), jnp.float32)
    for c in range(CHUNKS):
        rows = [jnp.zeros((4, LANES), jnp.float32)] * 3
        for i in range(CLUS):
            low = LANES * (c + 1) - PIECE * (i + 1)
            high = low + PIECE
            if high <= 0 or low >= LANES:
                continue
            inside = (lane >= low) & (lane < high)
            piece = pieces[i]
            for a in range(3):
                moved = pltpu.roll(piece, (low - PIECE * a) % LANES, 1)
                rows[a] = jnp.where(inside, moved, rows[a])
        for a in range(3):
            record[c, 4 * a : 4 * a + 4, :] = rows[a]
        total = jnp.sum(rows[0] * rows[0] + rows[1] * rows[1] + rows[2] * rows[2], axis=0, keepdims=True)
        squares_v[c : c + 1, :] = total

    squares = squares_v[...]
    row_id = lax.broadcasted_iota(jnp.int32, (LANES, LANES), 0)
    col_id = lax.broadcasted_iota(jnp.int32, (LANES, LANES), 1)
    upto = jnp.where(row_id <= col_id, 1.0, 0.0).astype(jnp.float32)
    prefix = jnp.dot(squares, upto, precision=lax.Precision.HIGHEST, preferred_element_type=jnp.float32)
    energy = []
    for h in range(2):
        whole = jnp.sum(prefix[h + 1 : h + 9, LANES - 1 : LANES], axis=0, keepdims=True)
        energy.append(prefix[h : h + 1, :] + (whole - prefix[h + 8 : h + 9, :]))

    near = row_id <= col_id
    none = jnp.zeros((SLOTS * RANK, LANES), jnp.bfloat16)
    captured = jnp.zeros((2 * SLOTS * RANK, LANES), jnp.float32)
    for j in range(CHANS):
        rolled = None
        for c in range(CHUNKS):
            later = pltpu.roll(
                jnp.broadcast_to(record[c, j : j + 1, :], (LANES, LANES)), 0, 1, stride=1, stride_axis=0
            )
            if c > 0:
                block = jnp.where(near, rolled, later)
                hankel[j, LANES * (c - 1) : LANES * c, :] = block.astype(jnp.bfloat16)
            rolled = later
        vectors = basis_v[lax.rem(slot_s[j], CHANS)]
        halves = jnp.concatenate(
            [jnp.concatenate([vectors, none], axis=1), jnp.concatenate([none, vectors], axis=1)], axis=0
        )
        projected = jnp.dot(halves, hankel[j], preferred_element_type=jnp.float32)
        captured = captured + projected * projected

    rank_id = lax.broadcasted_iota(jnp.int32, (RANK, LANES), 0)
    tx_a[...] = jnp.zeros((X, 4, LANES), jnp.float32)
    for p in range(SLOTS):
        for h in range(2):
            first = RANK * (SLOTS * h + p)
            part = jnp.where(rank_id < ranks[p], captured[first : first + RANK, :], 0.0)
            row = jnp.sum(part, axis=0, keepdims=True)
            for v in range(X):
                start = 32 * (X - 1 - v)
                tx_a[v, h : h + 1, 32 * p : 32 * (p + 1)] = row[:, start : start + 32]
    for h in range(2):
        for v in range(X):
            start = 32 * (X - 1 - v)
            tx_a[v, 2:3, 32 * h : 32 * (h + 1)] = energy[h][:, start : start + 32]

    for dx, dc in X_STEPS:
        pltpu.make_async_remote_copy(
            src_ref=tx_a.at[(x + dx) % X], dst_ref=rx_a.at[X * core + x], send_sem=send_a, recv_sem=recv_a,
            device_id=(chan_at(0, dx), clus_at(0, 0, dc)), device_id_type=MESH,
        ).start()
    rx_a[X * core + x] = tx_a[x]
    pltpu.make_async_copy(rx_a.at[pl.ds(0, len(X_STEPS))], rx_a.at[pl.ds(0, len(X_STEPS))], recv_a).wait()

    for c in range(CORE):
        first = X * c
        reduced = (rx_a[first] + rx_a[first + 1]) + (rx_a[first + 2] + rx_a[first + 3])
        for h in range(Z_HI):
            tx_b[h, c] = reduced[h : h + 1, :]
    tx_e[...] = reduced[2:3, :]
    energy_copy = pltpu.make_async_remote_copy(
        src_ref=tx_e, dst_ref=rx_e, send_sem=send_e, recv_sem=recv_e,
        device_id=(chan_at(1, 0), clus), device_id_type=MESH,
    )
    energy_copy.start()
    held_at = z_hi * CLUS + clus - core
    for dh, dz, dy in chip_steps():
        pltpu.make_async_remote_copy(
            src_ref=tx_b.at[(z_hi + dh) % Z_HI], dst_ref=rx_b.at[pl.ds(held_at, CORE)], send_sem=send_b, recv_sem=recv_b,
            device_id=(chan_at(dh, 0), clus_at(dz, dy, 0)), device_id_type=MESH,
        ).start()
    rx_b[pl.ds(held_at, CORE)] = tx_b[z_hi]
    energy_copy.wait_recv()
    both = reduced[2:3, :] + rx_e[...]
    energy_own = jnp.where(z_hi == 0, both[:, 0:32], both[:, 32:64]) + 1e-6
    pltpu.make_async_copy(rx_b.at[pl.ds(0, Z_HI * CLUS - CORE)], rx_b.at[pl.ds(0, Z_HI * CLUS - CORE)], recv_b).wait()
    for q in range(2):
        row = rx_b[own_holder[q]] + rx_b[CLUS + own_holder[q]]
        value = jnp.zeros((1, 32), jnp.float32)
        for p in range(SLOTS):
            value = jnp.where(positions[q] == p, row[:, 32 * p : 32 * (p + 1)], value)
        out_ref[q : q + 1, :] = (WINDOW / RANK) * value / energy_own

    pltpu.make_async_copy(pieces.at[pl.ds(0, CLUS - 1)], pieces.at[pl.ds(0, CLUS - 1)], send_1).wait()
    pltpu.make_async_copy(rx_a.at[pl.ds(0, len(X_STEPS))], rx_a.at[pl.ds(0, len(X_STEPS))], send_a).wait()
    pltpu.make_async_copy(rx_b.at[pl.ds(0, Z_HI * CLUS - CORE)], rx_b.at[pl.ds(0, Z_HI * CLUS - CORE)], send_b).wait()
    energy_copy.wait_send()


def local(waveform, basis_slots, slot_channel, cluster_holder, basis_count):
    basis = basis_slots.reshape(CHANS, SLOTS * RANK, WINDOW)
    f32 = jnp.float32
    latest_first = pl.pallas_call(
        kernel,
        out_shape=jax.ShapeDtypeStruct((2, 32), f32),
        in_specs=[pl.BlockSpec(memory_space=pltpu.HBM)] * 5,
        out_specs=pl.BlockSpec(memory_space=pltpu.VMEM),
        scratch_shapes=[
            pltpu.VMEM((CHANS, PIECE), f32),
            pltpu.VMEM((CHANS, SLOTS * RANK, WINDOW), jnp.bfloat16),
            pltpu.SMEM((CHANS,), jnp.int32),
            pltpu.SMEM((CLUSTERS,), jnp.int32),
            pltpu.SMEM((CLUSTERS,), jnp.int32),
            pltpu.VMEM((CLUS, 4, LANES), f32),
            pltpu.VMEM((CHUNKS, 16, LANES), f32),
            pltpu.VMEM((CHANS, HANKELS * LANES, LANES), jnp.bfloat16),
            pltpu.VMEM((16, LANES), f32),
            pltpu.VMEM((X, 4, LANES), f32),
            pltpu.VMEM((CORE * X, 4, LANES), f32),
            pltpu.VMEM((Z_HI, CORE, 1, LANES), f32),
            pltpu.VMEM((Z_HI * CLUS, 1, LANES), f32),
            pltpu.VMEM((1, LANES), f32),
            pltpu.VMEM((1, LANES), f32),
            pltpu.SemaphoreType.DMA((5,)),
            *[pltpu.SemaphoreType.DMA] * 8,
        ],
        compiler_params=pltpu.CompilerParams(collective_id=0, has_side_effects=True, vmem_limit_bytes=16<<20),
    )(*[pltpu.with_memory_space_constraint(a, pltpu.HBM) for a in (waveform, basis, slot_channel, cluster_holder, basis_count)])
    return latest_first[:, ::-1]


def solution(mesh):
    placed = (P("chan", "clus"), P("chan", "clus", None, None), P("chan"), P(), P())
    return jax.shard_map(
        local, mesh=mesh, in_specs=placed, out_specs=P("clus", "chan"), check_vma=False
    )
```
